32 devices in a mesh: tm: 8 (over y, x, core), freq: 4 (over z).
Axes of the slice: x: 2, y: 2, z: 4, core: 2. Of those that a mesh axis runs over, the one named last changes fastest.
Arguments:
- sfts: float32 [384, 2, 4096], P('tm', None, 'freq'), may hold values from -40 to 40
- detector_ids: int32 [384], replicated, may hold values from 0 to 2
- intersection: float32 [3, 3], replicated, may hold values from 0.3 to 1
- lags: int32 [12], replicated, may hold values from 1 to 16, as said below
- template_ids: int32 [4096, 2], P('tm'), may hold values from 0 to 63
Outputs:
- stat: float32 [4096, 4096], P('tm', 'freq')
The draws below stay inside these ranges and needn't reach their ends.
Inputs may be any that keep to these rules, and one draw needn't show every extreme that they name: 12 distinct lags, one of them 16.
All inputs are finite; a program needn't handle non-finite values.
Results may differ from the reference program's by a relative error of at most 0.009.
Values may be sent and summed in bfloat16 or wider, within the bound.
A program may use at most 64 MiB of HBM per device.

```python
import math
import jax
import jax.numpy as jnp
from jax import lax

NBIN = 4096
NTEMPL = 4096
LAGMAX = 16
NLAG = 12
NDET = 3
NGRID = 64
PERIOD = 283
SFT_DEV = 48
NSFT = 384


def draw_sfts(key, part):
    key_base = jax.random.fold_in(key, 11)
    key_rough = jax.random.fold_in(key, 12)
    key_rows = jax.random.fold_in(key, 13)
    bins = jnp.arange(NBIN, dtype=jnp.float32)
    ramp = jnp.exp(0.55 * bins / NBIN)
    rough = jax.random.uniform(key_rough, (NBIN,), jnp.float32, 0.6, 1.4)
    base = jnp.clip(jax.random.normal(key_base, (NSFT, 2, NBIN), jnp.float32), -6.0, 6.0)
    row_scale = jnp.exp(jax.random.uniform(key_rows, (NSFT,), jnp.float32, math.log(0.5), math.log(2.0)))
    values = base * row_scale[:, None, None] * (ramp * rough)[None, None, :]
    return jnp.clip(values, -40.0, 40.0).astype(jnp.float32)


def draw_lags(key, part):
    order = jax.random.permutation(jax.random.fold_in(key, 21), LAGMAX - 1)[:NLAG - 1].astype(jnp.int32) + 1
    return jnp.concatenate([jnp.full((1,), LAGMAX, jnp.int32), order])


def place_ends(array, stream_key, least, largest):
    longest = array.shape.index(max(array.shape))
    spots = []
    for shift in (0, 1):
        where = [jax.random.randint(jax.random.fold_in(stream_key, axis), (), 0, length) for axis, length in enumerate(array.shape)]
        where[longest] = (where[longest] + shift) % array.shape[longest]
        spots.append(tuple(where))
    return array.at[spots[0]].set(least).at[spots[1]].set(largest)


def setup_inputs(seed: int = 0) -> dict:
    key_list = jax.random.split(jax.random.key(seed), 6)
    sfts = draw_sfts(jax.random.fold_in(key_list[5], 71), 0)
    detector_ids = place_ends(jax.random.randint(key_list[1], (NSFT,), 0, NDET), jax.random.fold_in(key_list[1], 1), 0, NDET - 1).astype(jnp.int32)
    intersection = jnp.clip(jax.random.uniform(key_list[2], (NDET, NDET), jnp.float32, 0.3, 1.0), 0.3, 1.0)
    lags = draw_lags(jax.random.fold_in(key_list[5], 71), 0)
    template_ids = place_ends(jax.random.randint(key_list[4], (NTEMPL, 2), 0, NGRID), jax.random.fold_in(key_list[4], 1), 0, NGRID - 1).astype(jnp.int32)
    return {"sfts": sfts, "detector_ids": detector_ids, "intersection": intersection, "lags": lags, "template_ids": template_ids}


def block_term(extended, first_row, ids_padded, lag_list, intersection, amplitude_idx, phase_idx, total):
    span = extended.shape[0] - LAGMAX
    here = jnp.arange(span, dtype=jnp.int32)
    partner = here[None, :] + lag_list[:, None]
    own_rows = extended[:span].astype(jnp.float32)
    far_rows = extended[partner].astype(jnp.float32)
    det_block = lax.dynamic_slice_in_dim(ids_padded, first_row, extended.shape[0], 0)
    det_near = det_block[:span]
    det_far = det_block[partner]
    levels = jnp.arange(intersection.shape[0], dtype=jnp.int32)
    hot_near = (det_near[:, None] == levels[None, :]).astype(jnp.float32)
    hot_far = (det_far[:, :, None] == levels[None, None, :]).astype(jnp.float32)
    weight = jnp.einsum('sa,ab,lsb->ls', hot_near, intersection.astype(jnp.float32), hot_far)
    inside = first_row + partner < total
    weight = jnp.where(inside, weight, jnp.float32(0.0))
    re_own = own_rows[None, :, 0]
    im_own = own_rows[None, :, 1]
    re_far = far_rows[:, :, 0]
    im_far = far_rows[:, :, 1]
    pair_re = (weight[:, :, None] * (re_own * re_far + im_own * im_far)).astype(jnp.bfloat16)
    pair_im = (weight[:, :, None] * (re_own * im_far - im_own * re_far)).astype(jnp.bfloat16)
    width = extended.shape[2]
    stacked = jnp.concatenate([pair_re.reshape(-1, width), pair_im.reshape(-1, width)], 0)
    position = first_row + jnp.arange(extended.shape[0], dtype=jnp.int32)
    orbit = 2.0 * math.pi / PERIOD * (position % PERIOD).astype(jnp.float32)
    offset = 2.0 * math.pi / NGRID * phase_idx.astype(jnp.float32)
    sine = jnp.sin(offset[:, None] + orbit[None, :])
    amplitude = 8.0 + 4.0 * amplitude_idx.astype(jnp.float32)
    phase = amplitude[:, None, None] * (sine[:, partner] - sine[:, None, :span])
    rows = phase.shape[0]
    factors = jnp.concatenate([jnp.cos(phase).reshape(rows, -1).astype(jnp.bfloat16), jnp.sin(phase).reshape(rows, -1).astype(jnp.bfloat16)], 1)
    return jnp.dot(factors, stacked, preferred_element_type=jnp.float32)

def reference(sfts, detector_ids, intersection, lags, template_ids):
    power = lax.optimization_barrier(jnp.sum(sfts[:, 0] * sfts[:, 0] + sfts[:, 1] * sfts[:, 1], axis=1)) / NBIN
    white = (sfts * lax.rsqrt(power + 1e-06)[:, None, None]).astype(jnp.bfloat16)
    padded = jnp.pad(white, ((0, LAGMAX), (0, 0), (0, 0)))
    ids_padded = jnp.pad(detector_ids, (0, LAGMAX))
    total = sfts.shape[0]

    def add_block(number, totals):
        first_row = (number * SFT_DEV).astype(jnp.int32)
        extended = lax.dynamic_slice_in_dim(padded, first_row, SFT_DEV + LAGMAX, 0)
        return totals + block_term(extended, first_row, ids_padded, lags, intersection, template_ids[:, 0], template_ids[:, 1], total)
    totals = lax.fori_loop(0, total // SFT_DEV, add_block, jnp.zeros((NTEMPL, NBIN), jnp.float32))
    return totals * jnp.float32(1.0 / math.sqrt(total * NLAG))
```

```python
import functools
import math

import jax
import jax.numpy as jnp
import numpy as np
from jax import lax
from jax.experimental import pallas as pl
from jax.experimental.pallas import tpu as pltpu
from jax.sharding import PartitionSpec as P

NBIN = 4096
LAGMAX = 16
NGRID = 64
PERIOD = 283
PIECE = 256
CHUNK = 96
MESH = pl.DeviceIdType.MESH


def even_series(function, degree):
    nodes = np.cos(np.pi * (np.arange(64) + 0.5) / 64) * 0.125 + 0.125
    fit = np.polynomial.chebyshev.Chebyshev.fit(nodes, function(np.sqrt(nodes)), degree, domain=[0, 0.25])
    return [float(c) for c in fit.convert(kind=np.polynomial.Polynomial).coef]


SIN_SERIES = even_series(lambda y: np.sin(2 * np.pi * y) / y, 6)
COS_SERIES = even_series(lambda y: np.cos(2 * np.pi * y), 7)


def horner(series, z):
    value = jnp.full_like(z, series[-1])
    for coefficient in series[-2::-1]:
        value = value * z + coefficient
    return value


def turn_cos_sin(turns):
    y = turns - jnp.round(turns)
    z = y * y
    return horner(COS_SERIES, z), y * horner(SIN_SERIES, z)


def xor(index, bits):
    out = index
    bit = 1
    while bit <= bits:
        if bits & bit:
            out = out + bit - 2 * bit * ((index // bit) % 2)
        bit *= 2
    return out


def kernel(
    n, nf, scale,
    x_ref, det_ref, inter_ref, lag_ref, tid_ref, out_ref,
    buf, pbuf, rbuf, rcol, detcol, table, factors, white, pairs,
    bulk_send, bulk_recv, p_send, p_recv, r_send, r_recv,
):
    me = lax.axis_index("tm")
    mf = lax.axis_index("freq")
    span = x_ref.shape[0]
    rows = n * span
    nlag = lag_ref.shape[0]
    pieces = buf.shape[0]
    templ = tid_ref.shape[1]
    evens = [o for o in range(2, n, 2)]

    re = x_ref[:, 0, :]
    im = x_ref[:, 1, :]
    for p in range(pieces):
        cols = slice(p * PIECE, (p + 1) * PIECE)
        buf[p, me, 0] = re[:, cols].astype(jnp.bfloat16)
        buf[p, me, 1] = im[:, cols].astype(jnp.bfloat16)
    local = jnp.sum(re * re + im * im, axis=1, keepdims=True)
    eye = lax.broadcasted_iota(jnp.int32, (span, 128), 0) == lax.broadcasted_iota(jnp.int32, (span, 128), 1)
    local_row = jnp.sum(jnp.where(eye, local, 0.0), axis=0, keepdims=True)
    pbuf[0] = jnp.broadcast_to(local_row, (8, 128))

    barrier = pltpu.get_barrier_semaphore()
    for d in range(1, nf):
        pl.semaphore_signal(barrier, inc=1, device_id=(me, (mf + d) % nf), device_id_type=MESH)
    for o in range(1, n):
        pl.semaphore_signal(barrier, inc=1, device_id=(xor(me, o), mf), device_id_type=MESH)
    pl.semaphore_wait(barrier, nf - 1 + n - 1)

    def power_copy(d):
        return pltpu.make_async_remote_copy(
            src_ref=pbuf.at[0], dst_ref=pbuf.at[d], send_sem=p_send.at[d], recv_sem=p_recv.at[d],
            device_id=(me, (mf + d) % nf), device_id_type=MESH)

    def rate_copy(o):
        return pltpu.make_async_remote_copy(
            src_ref=rbuf.at[me], dst_ref=rbuf.at[me], send_sem=r_send.at[o], recv_sem=r_recv.at[o],
            device_id=(xor(me, o), mf), device_id_type=MESH)

    def own_copy(p, o):
        return pltpu.make_async_remote_copy(
            src_ref=buf.at[p, me], dst_ref=buf.at[p, me], send_sem=bulk_send.at[p, o], recv_sem=bulk_recv.at[p, o],
            device_id=(xor(me, o), mf), device_id_type=MESH)

    def pass_copy(p, o):
        block = xor(me, o)
        return pltpu.make_async_remote_copy(
            src_ref=buf.at[p, block], dst_ref=buf.at[p, block],
            send_sem=bulk_send.at[p, o + 1], recv_sem=bulk_recv.at[p, o + 1],
            device_id=(xor(me, 1), mf), device_id_type=MESH)

    def landed(p, o):
        block = xor(me, o)
        pltpu.make_async_remote_copy(
            src_ref=buf.at[p, block], dst_ref=buf.at[p, block],
            send_sem=bulk_send.at[p, o], recv_sem=bulk_recv.at[p, o],
            device_id=(xor(me, o), mf), device_id_type=MESH).wait_recv()

    for d in range(1, nf):
        power_copy(d).start()
    for p in range(pieces):
        for o in evens + [1]:
            own_copy(p, o).start()

    tail = rows + LAGMAX
    index = lax.broadcasted_iota(jnp.int32, (tail, 128), 0).astype(jnp.float32)
    position = index - PERIOD * jnp.floor((index + 0.5) * (1.0 / PERIOD))
    cos_i, sin_i = turn_cos_sin(position * (1.0 / PERIOD))
    for c in range(templ // 128):
        cols = slice(c * 128, (c + 1) * 128)
        cos_q, sin_q = turn_cos_sin(tid_ref[1:2, cols].astype(jnp.float32) * (1.0 / NGRID))
        amplitude = (8.0 + 4.0 * tid_ref[0:1, cols].astype(jnp.float32)) * (0.5 / math.pi)
        cos_t, sin_t = turn_cos_sin(amplitude * (sin_i * cos_q + cos_i * sin_q))
        table[0, c] = cos_t
        table[1, c] = sin_t

    for d in range(1, nf):
        power_copy(d).wait_recv()
    total = pbuf[0]
    for d in range(1, nf):
        total = total + pbuf[d]
    rbuf[me] = lax.rsqrt(total * (1.0 / NBIN) + 1e-06)

    square = lax.broadcasted_iota(jnp.int32, (128, 128), 0) == lax.broadcasted_iota(jnp.int32, (128, 128), 1)
    for c in range(rows // 128):
        ids = det_ref[0:1, c * 128:(c + 1) * 128].astype(jnp.float32)
        column = jnp.sum(jnp.where(square, ids, 0.0), axis=1, keepdims=True)
        detcol[c * 128:(c + 1) * 128, :] = jnp.broadcast_to(column, (128, 128))
    detcol[rows:tail, :] = jnp.full((LAGMAX, 128), -1.0, jnp.float32)
    white[:, :, rows:tail, :] = jnp.zeros((2, PIECE // 128, LAGMAX, 128), jnp.float32)

    for o in range(1, n):
        rate_copy(o).start()

    ndet = inter_ref.shape[0]
    block = 128

    def factor_step(l, carry):
        lag = lag_ref[l]
        for r in range(rows // block):
            here = slice(r * block, (r + 1) * block)
            there = pl.ds(r * block + lag, block)
            near = detcol[here, :]
            far = detcol[there, :]
            weight = jnp.zeros((block, 128), jnp.float32)
            for b in range(ndet):
                gain = jnp.zeros((block, 128), jnp.float32)
                for a in range(ndet):
                    gain = jnp.where(near == a, inter_ref[a, b], gain)
                weight = jnp.where(far == b, gain, weight)
            for c in range(templ // 128):
                cols = slice(c * 128, (c + 1) * 128)
                ci = table[0, c, here, :] * weight
                si = table[1, c, here, :] * weight
                cj = table[0, c, there, :]
                sj = table[1, c, there, :]
                cosine = (ci * cj + si * sj).T.astype(jnp.bfloat16)
                sine = (ci * sj - si * cj).T.astype(jnp.bfloat16)
                start = pl.multiple_of(2 * rows * l + r * block, 128)
                factors[cols, pl.ds(start, block)] = cosine
                factors[cols, pl.ds(start + rows, block)] = sine
        return carry

    def forward(p):
        for o in evens:
            landed(p, o)
            pass_copy(p, o).start()

    half = nlag // 2
    lax.fori_loop(0, half, factor_step, 0)
    forward(0)
    lax.fori_loop(half, nlag, factor_step, 0)

    for o in range(1, n):
        rate_copy_in = pltpu.make_async_remote_copy(
            src_ref=rbuf.at[xor(me, o)], dst_ref=rbuf.at[xor(me, o)], send_sem=r_send.at[o], recv_sem=r_recv.at[o],
            device_id=(xor(me, o), mf), device_id_type=MESH)
        rate_copy_in.wait_recv()
    for g in range(n):
        column = jnp.sum(jnp.where(eye, rbuf[g, 0:1, :], 0.0), axis=1, keepdims=True)
        rcol[g * span:(g + 1) * span, :] = jnp.broadcast_to(column, (span, 128))

    def piece_step(p, carry):
        for o in range(1, n, 2):
            landed(p, o)

        @pl.when(p + 1 < pieces)
        def _():
            forward(p + 1)

        for g in range(n):
            here = slice(g * span, (g + 1) * span)
            rate = rcol[here, :]
            for c in range(2):
                for h in range(PIECE // 128):
                    white[c, h, here, :] = buf[p, g, c, :, h * 128:(h + 1) * 128].astype(jnp.float32) * rate

        def pair_step(l, inner):
            lag = lag_ref[l]
            for r in range(rows // CHUNK):
                here = slice(r * CHUNK, (r + 1) * CHUNK)
                there = pl.ds(r * CHUNK + lag, CHUNK)
                start = pl.multiple_of(2 * rows * l + r * CHUNK, 32)
                for h in range(PIECE // 128):
                    cols = slice(h * 128, (h + 1) * 128)
                    a = white[0, h, here, :]
                    b = white[1, h, here, :]
                    c = white[0, h, there, :]
                    d = white[1, h, there, :]
                    pairs[pl.ds(start, CHUNK), cols] = (a * c + b * d).astype(jnp.bfloat16)
                    pairs[pl.ds(start + rows, CHUNK), cols] = (a * d - b * c).astype(jnp.bfloat16)
            return inner

        lax.fori_loop(0, nlag, pair_step, 0)
        product = jnp.dot(factors[...], pairs[...], preferred_element_type=jnp.float32)
        out_ref[:, pl.ds(pl.multiple_of(p * PIECE, PIECE), PIECE)] = product * scale
        return carry

    lax.fori_loop(0, pieces, piece_step, 0)

    for d in range(1, nf):
        power_copy(d).wait_send()
    for o in range(1, n):
        rate_copy(o).wait_send()

    def drain(p, carry):
        for o in evens + [1]:
            own_copy(p, o).wait_send()
        for o in evens:
            pass_copy(p, o).wait_send()
        return carry

    lax.fori_loop(0, pieces, drain, 0)


def shards(n, nf, sfts, detector_ids, intersection, lags, template_ids):
    span, _, width = sfts.shape
    rows = detector_ids.shape[0]
    nlag = lags.shape[0]
    templ = template_ids.shape[0]
    pieces = width // PIECE
    vmem = pl.BlockSpec(memory_space=pltpu.VMEM)
    smem = pl.BlockSpec(memory_space=pltpu.SMEM)
    scale = 1.0 / math.sqrt(rows * nlag)
    return pl.pallas_call(
        functools.partial(kernel, n, nf, scale),
        out_shape=jax.ShapeDtypeStruct((templ, width), jnp.float32),
        in_specs=[vmem, vmem, smem, smem, vmem],
        out_specs=vmem,
        scratch_shapes=[
            pltpu.VMEM((pieces, n, 2, span, PIECE), jnp.bfloat16),
            pltpu.VMEM((nf, 8, 128), jnp.float32),
            pltpu.VMEM((n, 8, 128), jnp.float32),
            pltpu.VMEM((rows, 128), jnp.float32),
            pltpu.VMEM((rows + LAGMAX, 128), jnp.float32),
            pltpu.VMEM((2, templ // 128, rows + LAGMAX, 128), jnp.float32),
            pltpu.VMEM((templ, 2 * rows * nlag), jnp.bfloat16),
            pltpu.VMEM((2, PIECE // 128, rows + LAGMAX, 128), jnp.float32),
            pltpu.VMEM((2 * rows * nlag, PIECE), jnp.bfloat16),
            pltpu.SemaphoreType.DMA((pieces, n)),
            pltpu.SemaphoreType.DMA((pieces, n)),
            pltpu.SemaphoreType.DMA((nf,)),
            pltpu.SemaphoreType.DMA((nf,)),
            pltpu.SemaphoreType.DMA((n,)),
            pltpu.SemaphoreType.DMA((n,)),
        ],
        compiler_params=pltpu.CompilerParams(
            collective_id=0, has_side_effects=True, vmem_limit_bytes=60 * 1024 * 1024
        ),
    )(sfts, detector_ids.reshape(1, rows), intersection, lags, template_ids.T)


def solution(mesh):
    n, nf = mesh.shape["tm"], mesh.shape["freq"]
    in_specs = (P("tm", None, "freq"), P(), P(), P(), P("tm", None))
    return jax.shard_map(
        functools.partial(shards, n, nf), mesh=mesh, in_specs=in_specs, out_specs=P("tm", "freq"), check_vma=False
    )
```

```python
import functools
import math

import jax
import jax.numpy as jnp
import numpy as np
from jax import lax
from jax.experimental import pallas as pl
from jax.experimental.pallas import tpu as pltpu
from jax.sharding import PartitionSpec as P

NBIN = 4096
LAGMAX = 16
NGRID = 64
PERIOD = 283
PIECE = 256
CHUNK = 32
GROUP = 2
MESH = pl.DeviceIdType.MESH


def even_series(function, degree):
    nodes = np.cos(np.pi * (np.arange(64) + 0.5) / 64) * 0.125 + 0.125
    fit = np.polynomial.chebyshev.Chebyshev.fit(nodes, function(np.sqrt(nodes)), degree, domain=[0, 0.25])
    return [float(c) for c in fit.convert(kind=np.polynomial.Polynomial).coef]


SIN_SERIES = even_series(lambda y: np.sin(2 * np.pi * y) / y, 6)
COS_SERIES = even_series(lambda y: np.cos(2 * np.pi * y), 7)


def horner(series, z):
    value = jnp.full_like(z, series[-1])
    for coefficient in series[-2::-1]:
        value = value * z + coefficient
    return value


def turn_cos_sin(turns):
    y = turns - jnp.round(turns)
    z = y * y
    return horner(COS_SERIES, z), y * horner(SIN_SERIES, z)


def xor(index, bits):
    out = index
    bit = 1
    while bit <= bits:
        if bits & bit:
            out = out + bit - 2 * bit * ((index // bit) % 2)
        bit *= 2
    return out


def kernel(
    n, nf, scale,
    x_ref, det_ref, inter_ref, lag_ref, tid_ref, out_ref,
    buf, pbuf, rbuf, rcol, detcol, weights, table, turned, factors, white, pairs_a, pairs_b, acc,
    bulk_send, bulk_recv, p_send, p_recv, r_send, r_recv,
):
    me = lax.axis_index("tm")
    mf = lax.axis_index("freq")
    span = x_ref.shape[0]
    rows = n * span
    nlag = lag_ref.shape[0]
    pieces = buf.shape[0]
    templ = tid_ref.shape[1]
    kept = weights.shape[2]
    terms = weights.shape[1]
    tail = detcol.shape[0]
    groups = nlag // GROUP
    depth = 2 * kept * GROUP
    evens = [o for o in range(2, n, 2)]

    re = x_ref[:, 0, :]
    im = x_ref[:, 1, :]
    for p in range(pieces):
        cols = slice(p * PIECE, (p + 1) * PIECE)
        buf[p, me, 0] = re[:, cols].astype(jnp.bfloat16)
        buf[p, me, 1] = im[:, cols].astype(jnp.bfloat16)
    local = jnp.sum(re * re + im * im, axis=1, keepdims=True)
    eye = lax.broadcasted_iota(jnp.int32, (span, 128), 0) == lax.broadcasted_iota(jnp.int32, (span, 128), 1)
    local_row = jnp.sum(jnp.where(eye, local, 0.0), axis=0, keepdims=True)
    pbuf[0] = jnp.broadcast_to(local_row, (8, 128))

    barrier = pltpu.get_barrier_semaphore()
    for d in range(1, nf):
        pl.semaphore_signal(barrier, inc=1, device_id=(me, (mf + d) % nf), device_id_type=MESH)
    for o in range(1, n):
        pl.semaphore_signal(barrier, inc=1, device_id=(xor(me, o), mf), device_id_type=MESH)
    pl.semaphore_wait(barrier, nf - 1 + n - 1)

    def power_copy(d):
        return pltpu.make_async_remote_copy(
            src_ref=pbuf.at[0], dst_ref=pbuf.at[d], send_sem=p_send.at[d], recv_sem=p_recv.at[d],
            device_id=(me, (mf + d) % nf), device_id_type=MESH)

    def rate_copy(o):
        return pltpu.make_async_remote_copy(
            src_ref=rbuf.at[me], dst_ref=rbuf.at[me], send_sem=r_send.at[o], recv_sem=r_recv.at[o],
            device_id=(xor(me, o), mf), device_id_type=MESH)

    def own_copy(p, o):
        return pltpu.make_async_remote_copy(
            src_ref=buf.at[p, me], dst_ref=buf.at[p, me], send_sem=bulk_send.at[p, o], recv_sem=bulk_recv.at[p, o],
            device_id=(xor(me, o), mf), device_id_type=MESH)

    def pass_copy(p, o):
        block = xor(me, o)
        return pltpu.make_async_remote_copy(
            src_ref=buf.at[p, block], dst_ref=buf.at[p, block],
            send_sem=bulk_send.at[p, o + 1], recv_sem=bulk_recv.at[p, o + 1],
            device_id=(xor(me, 1), mf), device_id_type=MESH)

    def landed(p, o):
        block = xor(me, o)
        pltpu.make_async_remote_copy(
            src_ref=buf.at[p, block], dst_ref=buf.at[p, block],
            send_sem=bulk_send.at[p, o], recv_sem=bulk_recv.at[p, o],
            device_id=(xor(me, o), mf), device_id_type=MESH).wait_recv()

    for d in range(1, nf):
        power_copy(d).start()
    for p in range(pieces):
        for o in evens + [1]:
            own_copy(p, o).start()

    index = lax.broadcasted_iota(jnp.int32, (kept + LAGMAX, 128), 0).astype(jnp.float32)
    position = index - PERIOD * jnp.floor((index + 0.5) * (1.0 / PERIOD))
    cos_i, sin_i = turn_cos_sin(position * (1.0 / PERIOD))
    for c in range(templ // 128):
        cols = slice(c * 128, (c + 1) * 128)
        cos_q, sin_q = turn_cos_sin(tid_ref[1:2, cols].astype(jnp.float32) * (1.0 / NGRID))
        amplitude = (8.0 + 4.0 * tid_ref[0:1, cols].astype(jnp.float32)) * (0.5 / math.pi)
        cos_t, sin_t = turn_cos_sin(amplitude * (sin_i * cos_q + cos_i * sin_q))
        table[0, c] = cos_t
        table[1, c] = sin_t

    square = lax.broadcasted_iota(jnp.int32, (128, 128), 0) == lax.broadcasted_iota(jnp.int32, (128, 128), 1)
    for c in range(rows // 128):
        ids = det_ref[c * 128:(c + 1) * 128].astype(jnp.float32)[None, :]
        column = jnp.sum(jnp.where(square, ids, 0.0), axis=1, keepdims=True)
        detcol[c * 128:(c + 1) * 128, :] = jnp.broadcast_to(column, (128, 128))
    detcol[rows:tail, :] = jnp.full((tail - rows, 128), -1.0, jnp.float32)
    white[:, :, rows:tail, :] = jnp.zeros((2, PIECE // 128, tail - rows, 128), jnp.float32)

    ndet = inter_ref.shape[0]
    level = lax.broadcasted_iota(jnp.int32, (kept, 128), 0) < PERIOD

    def weight_step(l, carry):
        lag = lag_ref[l]
        for m in range(terms):
            near = detcol[m * PERIOD:m * PERIOD + kept, :]
            far = detcol[pl.ds(m * PERIOD + lag, kept), :]
            weight = jnp.zeros((kept, 128), jnp.float32)
            for b in range(ndet):
                gain = jnp.zeros((kept, 128), jnp.float32)
                for a in range(ndet):
                    gain = jnp.where(near == a, inter_ref[a, b], gain)
                weight = jnp.where(far == b, gain, weight)
            weights[l, m] = jnp.where(level, weight, 0.0)
        return carry

    def factor_step(g, carry):
        for k in range(GROUP):
            lag = lag_ref[g * GROUP + k]
            for c in range(templ // 128):
                cols = slice(c * 128, (c + 1) * 128)
                ci = table[0, c, 0:kept, :]
                si = table[1, c, 0:kept, :]
                cj = table[0, c, pl.ds(lag, kept), :]
                sj = table[1, c, pl.ds(lag, kept), :]
                turned[2 * k * kept:(2 * k + 1) * kept, cols] = (ci * cj + si * sj).astype(jnp.bfloat16)
                turned[(2 * k + 1) * kept:(2 * k + 2) * kept, cols] = (ci * sj - si * cj).astype(jnp.bfloat16)
        for b in range(depth // 128):
            factors[g, :, b * 128:(b + 1) * 128] = turned[b * 128:(b + 1) * 128, :].T
        return carry

    def forward(p):
        for o in evens:
            landed(p, o)
            pass_copy(p, o).start()

    first = groups // 3
    second = 2 * groups // 3
    lax.fori_loop(0, first, factor_step, 0)
    for d in range(1, nf):
        power_copy(d).wait_recv()
    total = pbuf[0]
    for d in range(1, nf):
        total = total + pbuf[d]
    rbuf[me] = lax.rsqrt(total * (1.0 / NBIN) + 1e-06)

    for o in range(1, n):
        rate_copy(o).start()

    forward(0)
    lax.fori_loop(first, second, factor_step, 0)
    forward(1)
    lax.fori_loop(second, groups, factor_step, 0)
    lax.fori_loop(0, nlag, weight_step, 0)

    for o in range(1, n):
        rate_copy_in = pltpu.make_async_remote_copy(
            src_ref=rbuf.at[xor(me, o)], dst_ref=rbuf.at[xor(me, o)], send_sem=r_send.at[o], recv_sem=r_recv.at[o],
            device_id=(xor(me, o), mf), device_id_type=MESH)
        rate_copy_in.wait_recv()
    for g in range(n):
        column = jnp.sum(jnp.where(eye, rbuf[g, 0:1, :], 0.0), axis=1, keepdims=True)
        rcol[g * span:(g + 1) * span, :] = jnp.broadcast_to(column, (span, 128))

    def piece_step(p, carry):
        for o in range(1, n, 2):
            landed(p, o)

        @pl.when(p + 2 < pieces)
        def _():
            forward(p + 2)

        for g in range(n):
            here = slice(g * span, (g + 1) * span)
            rate = rcol[here, :]
            for c in range(2):
                for h in range(PIECE // 128):
                    white[c, h, here, :] = buf[p, g, c, :, h * 128:(h + 1) * 128].astype(jnp.float32) * rate

        def make_pairs(g, pairs):
            for r in range(0, kept, CHUNK):
                for k in range(GROUP):
                    l = g * GROUP + k
                    lag = lag_ref[l]
                    for h in range(PIECE // 128):
                        cols = slice(h * 128, (h + 1) * 128)
                        real = None
                        for m in range(terms):
                            if m * PERIOD + r >= rows:
                                continue
                            here = slice(m * PERIOD + r, m * PERIOD + r + CHUNK)
                            there = pl.ds(m * PERIOD + r + lag, CHUNK)
                            w = weights[l, m, r:r + CHUNK, :]
                            a = white[0, h, here, :]
                            b = white[1, h, here, :]
                            c = white[0, h, there, :]
                            d = white[1, h, there, :]
                            re_m = w * (a * c + b * d)
                            im_m = w * (a * d - b * c)
                            real = re_m if m == 0 else real + re_m
                            imag = im_m if m == 0 else imag + im_m
                        start = 2 * k * kept + r
                        pairs[start:start + CHUNK, cols] = real.astype(jnp.bfloat16)
                        pairs[start + kept:start + kept + CHUNK, cols] = imag.astype(jnp.bfloat16)

        slots = (pairs_a, pairs_b)
        make_pairs(0, slots[0])
        for g in range(groups):
            if g + 1 < groups:
                make_pairs(g + 1, slots[(g + 1) % 2])
            product = jnp.dot(factors[g], slots[g % 2][...], preferred_element_type=jnp.float32)
            if g == 0:
                acc[...] = product
            elif g + 1 < groups:
                acc[...] += product
            else:
                cols = pl.ds(pl.multiple_of(p * PIECE, PIECE), PIECE)
                out_ref[:, cols] = ((acc[...] + product) * scale).astype(out_ref.dtype)
        return carry

    lax.fori_loop(0, pieces, piece_step, 0)

    for d in range(1, nf):
        power_copy(d).wait_send()
    for o in range(1, n):
        rate_copy(o).wait_send()

    def drain(p, carry):
        for o in evens + [1]:
            own_copy(p, o).wait_send()
        for o in evens:
            pass_copy(p, o).wait_send()
        return carry

    lax.fori_loop(0, pieces, drain, 0)


def shards(n, nf, sfts, detector_ids, intersection, lags, template_ids):
    span, _, width = sfts.shape
    rows = detector_ids.shape[0]
    nlag = lags.shape[0]
    templ = template_ids.shape[0]
    pieces = width // PIECE
    kept = -(-PERIOD // CHUNK) * CHUNK
    terms = -(-rows // PERIOD)
    tail = (terms - 1) * PERIOD + kept + LAGMAX
    tail = -(-tail // 8) * 8
    depth = 2 * kept * GROUP
    vmem = pl.BlockSpec(memory_space=pltpu.VMEM)
    smem = pl.BlockSpec(memory_space=pltpu.SMEM)
    scale = 1.0 / math.sqrt(rows * nlag)
    stat = pl.pallas_call(
        functools.partial(kernel, n, nf, scale),
        out_shape=jax.ShapeDtypeStruct((templ, width), jnp.bfloat16),
        in_specs=[vmem, vmem, smem, smem, vmem],
        out_specs=vmem,
        scratch_shapes=[
            pltpu.VMEM((pieces, n, 2, span, PIECE), jnp.bfloat16),
            pltpu.VMEM((nf, 8, 128), jnp.float32),
            pltpu.VMEM((n, 8, 128), jnp.float32),
            pltpu.VMEM((rows, 128), jnp.float32),
            pltpu.VMEM((tail, 128), jnp.float32),
            pltpu.VMEM((nlag, terms, kept, 128), jnp.float32),
            pltpu.VMEM((2, templ // 128, kept + LAGMAX, 128), jnp.float32),
            pltpu.VMEM((depth, templ), jnp.bfloat16),
            pltpu.VMEM((nlag // GROUP, templ, depth), jnp.bfloat16),
            pltpu.VMEM((2, PIECE // 128, tail, 128), jnp.float32),
            pltpu.VMEM((depth, PIECE), jnp.bfloat16),
            pltpu.VMEM((depth, PIECE), jnp.bfloat16),
            pltpu.VMEM((templ, PIECE), jnp.float32),
            pltpu.SemaphoreType.DMA((pieces, n)),
            pltpu.SemaphoreType.DMA((pieces, n)),
            pltpu.SemaphoreType.DMA((nf,)),
            pltpu.SemaphoreType.DMA((nf,)),
            pltpu.SemaphoreType.DMA((n,)),
            pltpu.SemaphoreType.DMA((n,)),
        ],
        compiler_params=pltpu.CompilerParams(
            collective_id=0, has_side_effects=True, vmem_limit_bytes=36 * 1024 * 1024
        ),
    )(sfts, detector_ids, intersection, lags, template_ids.T)
    return stat.astype(jnp.float32)


def solution(mesh):
    n, nf = mesh.shape["tm"], mesh.shape["freq"]
    in_specs = (P("tm", None, "freq"), P(), P(), P(), P("tm", None))
    return jax.shard_map(
        functools.partial(shards, n, nf), mesh=mesh, in_specs=in_specs, out_specs=P("tm", "freq"), check_vma=False
    )
```

```python
import functools
import math

import jax
import jax.numpy as jnp
import numpy as np
from jax import lax
from jax.experimental import pallas as pl
from jax.experimental.pallas import tpu as pltpu
from jax.sharding import PartitionSpec as P

NBIN = 4096
LAGMAX = 16
NGRID = 64
PERIOD = 283
PIECE = 256
CHUNK = 96
MESH = pl.DeviceIdType.MESH


def even_series(function, degree):
    nodes = np.cos(np.pi * (np.arange(64) + 0.5) / 64) * 0.125 + 0.125
    fit = np.polynomial.chebyshev.Chebyshev.fit(nodes, function(np.sqrt(nodes)), degree, domain=[0, 0.25])
    return [float(c) for c in fit.convert(kind=np.polynomial.Polynomial).coef]


SIN_SERIES = even_series(lambda y: np.sin(2 * np.pi * y) / y, 6)
COS_SERIES = even_series(lambda y: np.cos(2 * np.pi * y), 7)


def horner(series, z):
    value = jnp.full_like(z, series[-1])
    for coefficient in series[-2::-1]:
        value = value * z + coefficient
    return value


def turn_cos_sin(turns):
    y = turns - jnp.round(turns)
    z = y * y
    return horner(COS_SERIES, z), y * horner(SIN_SERIES, z)


def xor(index, bits):
    out = index
    bit = 1
    while bit <= bits:
        if bits & bit:
            out = out + bit - 2 * bit * ((index // bit) % 2)
        bit *= 2
    return out


def kernel(
    n, nf, scale,
    x_ref, det_ref, inter_ref, lag_ref, tid_ref, out_ref,
    buf, pbuf, rbuf, rcol, detcol, table, factors, white, pairs,
    bulk_send, bulk_recv, p_send, p_recv, r_send, r_recv,
):
    me = lax.axis_index("tm")
    mf = lax.axis_index("freq")
    span = x_ref.shape[0]
    rows = n * span
    nlag = lag_ref.shape[0]
    pieces = buf.shape[0]
    templ = tid_ref.shape[1]
    evens = [o for o in range(2, n, 2)]

    re = x_ref[:, 0, :]
    im = x_ref[:, 1, :]
    for p in range(pieces):
        cols = slice(p * PIECE, (p + 1) * PIECE)
        buf[p, me, 0] = re[:, cols].astype(jnp.bfloat16)
        buf[p, me, 1] = im[:, cols].astype(jnp.bfloat16)
    local = jnp.sum(re * re + im * im, axis=1, keepdims=True)
    eye = lax.broadcasted_iota(jnp.int32, (span, 128), 0) == lax.broadcasted_iota(jnp.int32, (span, 128), 1)
    local_row = jnp.sum(jnp.where(eye, local, 0.0), axis=0, keepdims=True)
    pbuf[0] = jnp.broadcast_to(local_row, (8, 128))

    barrier = pltpu.get_barrier_semaphore()
    for d in range(1, nf):
        pl.semaphore_signal(barrier, inc=1, device_id=(me, (mf + d) % nf), device_id_type=MESH)
    for o in range(1, n):
        pl.semaphore_signal(barrier, inc=1, device_id=(xor(me, o), mf), device_id_type=MESH)
    pl.semaphore_wait(barrier, nf - 1 + n - 1)

    def power_copy(d):
        return pltpu.make_async_remote_copy(
            src_ref=pbuf.at[0], dst_ref=pbuf.at[d], send_sem=p_send.at[d], recv_sem=p_recv.at[d],
            device_id=(me, (mf + d) % nf), device_id_type=MESH)

    def rate_copy(o):
        return pltpu.make_async_remote_copy(
            src_ref=rbuf.at[me], dst_ref=rbuf.at[me], send_sem=r_send.at[o], recv_sem=r_recv.at[o],
            device_id=(xor(me, o), mf), device_id_type=MESH)

    def own_copy(p, o):
        return pltpu.make_async_remote_copy(
            src_ref=buf.at[p, me], dst_ref=buf.at[p, me], send_sem=bulk_send.at[p, o], recv_sem=bulk_recv.at[p, o],
            device_id=(xor(me, o), mf), device_id_type=MESH)

    def pass_copy(p, o):
        block = xor(me, o)
        return pltpu.make_async_remote_copy(
            src_ref=buf.at[p, block], dst_ref=buf.at[p, block],
            send_sem=bulk_send.at[p, o + 1], recv_sem=bulk_recv.at[p, o + 1],
            device_id=(xor(me, 1), mf), device_id_type=MESH)

    def landed(p, o):
        block = xor(me, o)
        pltpu.make_async_remote_copy(
            src_ref=buf.at[p, block], dst_ref=buf.at[p, block],
            send_sem=bulk_send.at[p, o], recv_sem=bulk_recv.at[p, o],
            device_id=(xor(me, o), mf), device_id_type=MESH).wait_recv()

    for d in range(1, nf):
        power_copy(d).start()
    for p in range(pieces):
        for o in evens + [1]:
            own_copy(p, o).start()

    tail = rows + LAGMAX
    index = lax.broadcasted_iota(jnp.int32, (tail, 128), 0).astype(jnp.float32)
    position = index - PERIOD * jnp.floor((index + 0.5) * (1.0 / PERIOD))
    cos_i, sin_i = turn_cos_sin(position * (1.0 / PERIOD))
    for c in range(templ // 128):
        cols = slice(c * 128, (c + 1) * 128)
        cos_q, sin_q = turn_cos_sin(tid_ref[1:2, cols].astype(jnp.float32) * (1.0 / NGRID))
        amplitude = (8.0 + 4.0 * tid_ref[0:1, cols].astype(jnp.float32)) * (0.5 / math.pi)
        cos_t, sin_t = turn_cos_sin(amplitude * (sin_i * cos_q + cos_i * sin_q))
        table[0, c] = cos_t
        table[1, c] = sin_t

    square = lax.broadcasted_iota(jnp.int32, (128, 128), 0) == lax.broadcasted_iota(jnp.int32, (128, 128), 1)
    for c in range(rows // 128):
        ids = det_ref[c * 128:(c + 1) * 128].astype(jnp.float32)[None, :]
        column = jnp.sum(jnp.where(square, ids, 0.0), axis=1, keepdims=True)
        detcol[c * 128:(c + 1) * 128, :] = jnp.broadcast_to(column, (128, 128))
    detcol[rows:tail, :] = jnp.full((LAGMAX, 128), -1.0, jnp.float32)
    white[:, :, rows:tail, :] = jnp.zeros((2, PIECE // 128, LAGMAX, 128), jnp.float32)

    ndet = inter_ref.shape[0]
    block = 128

    def factor_step(l, carry):
        lag = lag_ref[l]
        for r in range(rows // block):
            here = slice(r * block, (r + 1) * block)
            there = pl.ds(r * block + lag, block)
            near = detcol[here, :]
            far = detcol[there, :]
            weight = jnp.zeros((block, 128), jnp.float32)
            for b in range(ndet):
                gain = jnp.zeros((block, 128), jnp.float32)
                for a in range(ndet):
                    gain = jnp.where(near == a, inter_ref[a, b], gain)
                weight = jnp.where(far == b, gain, weight)
            for c in range(templ // 128):
                cols = slice(c * 128, (c + 1) * 128)
                ci = table[0, c, here, :] * weight
                si = table[1, c, here, :] * weight
                cj = table[0, c, there, :]
                sj = table[1, c, there, :]
                cosine = (ci * cj + si * sj).T.astype(jnp.bfloat16)
                sine = (ci * sj - si * cj).T.astype(jnp.bfloat16)
                start = pl.multiple_of(2 * rows * l + r * block, 128)
                factors[cols, pl.ds(start, block)] = cosine
                factors[cols, pl.ds(start + rows, block)] = sine
        return carry

    def forward(p):
        for o in evens:
            landed(p, o)
            pass_copy(p, o).start()

    half = nlag // 2
    lax.fori_loop(0, half, factor_step, 0)
    for d in range(1, nf):
        power_copy(d).wait_recv()
    total = pbuf[0]
    for d in range(1, nf):
        total = total + pbuf[d]
    rbuf[me] = lax.rsqrt(total * (1.0 / NBIN) + 1e-06)

    for o in range(1, n):
        rate_copy(o).start()

    forward(0)
    lax.fori_loop(half, nlag, factor_step, 0)

    for o in range(1, n):
        rate_copy_in = pltpu.make_async_remote_copy(
            src_ref=rbuf.at[xor(me, o)], dst_ref=rbuf.at[xor(me, o)], send_sem=r_send.at[o], recv_sem=r_recv.at[o],
            device_id=(xor(me, o), mf), device_id_type=MESH)
        rate_copy_in.wait_recv()
    for g in range(n):
        column = jnp.sum(jnp.where(eye, rbuf[g, 0:1, :], 0.0), axis=1, keepdims=True)
        rcol[g * span:(g + 1) * span, :] = jnp.broadcast_to(column, (span, 128))

    def piece_step(p, carry):
        for o in range(1, n, 2):
            landed(p, o)

        @pl.when(p + 1 < pieces)
        def _():
            forward(p + 1)

        for g in range(n):
            here = slice(g * span, (g + 1) * span)
            rate = rcol[here, :]
            for c in range(2):
                for h in range(PIECE // 128):
                    white[c, h, here, :] = buf[p, g, c, :, h * 128:(h + 1) * 128].astype(jnp.float32) * rate

        def pair_step(l, inner):
            lag = lag_ref[l]
            for r in range(rows // CHUNK):
                here = slice(r * CHUNK, (r + 1) * CHUNK)
                there = pl.ds(r * CHUNK + lag, CHUNK)
                start = pl.multiple_of(2 * rows * l + r * CHUNK, 32)
                for h in range(PIECE // 128):
                    cols = slice(h * 128, (h + 1) * 128)
                    a = white[0, h, here, :]
                    b = white[1, h, here, :]
                    c = white[0, h, there, :]
                    d = white[1, h, there, :]
                    pairs[pl.ds(start, CHUNK), cols] = (a * c + b * d).astype(jnp.bfloat16)
                    pairs[pl.ds(start + rows, CHUNK), cols] = (a * d - b * c).astype(jnp.bfloat16)
            return inner

        lax.fori_loop(0, nlag, pair_step, 0)
        product = jnp.dot(factors[...], pairs[...], preferred_element_type=jnp.float32)
        out_ref[:, pl.ds(pl.multiple_of(p * PIECE, PIECE), PIECE)] = (product * scale).astype(out_ref.dtype)
        return carry

    lax.fori_loop(0, pieces, piece_step, 0)

    for d in range(1, nf):
        power_copy(d).wait_send()
    for o in range(1, n):
        rate_copy(o).wait_send()

    def drain(p, carry):
        for o in evens + [1]:
            own_copy(p, o).wait_send()
        for o in evens:
            pass_copy(p, o).wait_send()
        return carry

    lax.fori_loop(0, pieces, drain, 0)


def shards(n, nf, sfts, detector_ids, intersection, lags, template_ids):
    span, _, width = sfts.shape
    rows = detector_ids.shape[0]
    nlag = lags.shape[0]
    templ = template_ids.shape[0]
    pieces = width // PIECE
    vmem = pl.BlockSpec(memory_space=pltpu.VMEM)
    smem = pl.BlockSpec(memory_space=pltpu.SMEM)
    scale = 1.0 / math.sqrt(rows * nlag)
    stat = pl.pallas_call(
        functools.partial(kernel, n, nf, scale),
        out_shape=jax.ShapeDtypeStruct((templ, width), jnp.bfloat16),
        in_specs=[vmem, vmem, smem, smem, vmem],
        out_specs=vmem,
        scratch_shapes=[
            pltpu.VMEM((pieces, n, 2, span, PIECE), jnp.bfloat16),
            pltpu.VMEM((nf, 8, 128), jnp.float32),
            pltpu.VMEM((n, 8, 128), jnp.float32),
            pltpu.VMEM((rows, 128), jnp.float32),
            pltpu.VMEM((rows + LAGMAX, 128), jnp.float32),
            pltpu.VMEM((2, templ // 128, rows + LAGMAX, 128), jnp.float32),
            pltpu.VMEM((templ, 2 * rows * nlag), jnp.bfloat16),
            pltpu.VMEM((2, PIECE // 128, rows + LAGMAX, 128), jnp.float32),
            pltpu.VMEM((2 * rows * nlag, PIECE), jnp.bfloat16),
            pltpu.SemaphoreType.DMA((pieces, n)),
            pltpu.SemaphoreType.DMA((pieces, n)),
            pltpu.SemaphoreType.DMA((nf,)),
            pltpu.SemaphoreType.DMA((nf,)),
            pltpu.SemaphoreType.DMA((n,)),
            pltpu.SemaphoreType.DMA((n,)),
        ],
        compiler_params=pltpu.CompilerParams(
            collective_id=0, has_side_effects=True, vmem_limit_bytes=60 * 1024 * 1024
        ),
    )(sfts, detector_ids, intersection, lags, template_ids.T)
    return stat.astype(jnp.float32)


def solution(mesh):
    n, nf = mesh.shape["tm"], mesh.shape["freq"]
    in_specs = (P("tm", None, "freq"), P(), P(), P(), P("tm", None))
    return jax.shard_map(
        functools.partial(shards, n, nf), mesh=mesh, in_specs=in_specs, out_specs=P("tm", "freq"), check_vma=False
    )
```
